32 devices in a mesh: rows: 8 (over z, y), rhs: 4 (over x, core).
Axes of the slice: x: 2, y: 2, z: 4, core: 2. Of those that a mesh axis runs over, the one named last changes fastest.
Arguments:
- upper_unit: float32 [128, 128, 128], P('rows'), may hold values from -1 to 1, as said below
- lower_unit: float32 [128, 128, 128], P('rows'), may hold values from -1 to 1, as said below
- pivot_inv: float32 [128, 128, 128], P('rows'), may hold values from -0.25 to 2.25
- loss_grad_one: float32 [128, 128, 128], P('rows', 'rhs'), may hold values from -6 to 6
- loss_grad_two: float32 [128, 128, 128], P('rows', 'rhs'), may hold values from -0.1875 to 0.1875
- state_one: float32 [128, 128, 128], P('rows', 'rhs'), may hold values from -0.01171875 to 0.01171875
- state_two: float32 [128, 128, 128], P('rows', 'rhs'), may hold values from -1.5 to 1.5
Outputs:
- operator_grad: float32 [128, 3, 128, 128], P('rhs', None, 'rows')
The draws below stay inside these ranges and needn't reach their ends.
Inputs may be any that keep to these rules, and one draw needn't show every extreme that they name: `upper_unit`: every block has spectral norm below 1. `lower_unit`: every block has spectral norm below 1.
All inputs are finite; a program needn't handle non-finite values.
Results may differ from the reference program's by a relative error of at most 0.0003.
Values sent between devices are 32-bit elements; how exact they have to be, the bound alone decides.
A program may use at most 128 MiB of HBM per device.

```python
import math
import jax
import jax.numpy as jnp
from jax import lax

CELL_COMPONENTS = 128
DIRECTIONS = 128
TOTAL_BLOCK_ROWS = 128


EXACT_ARITHMETIC = lax.Precision.HIGHEST


def chain_factors(key, salt_value):
    salted = jax.random.fold_in(key, salt_value)
    random_subkeys = jax.random.split(salted, 8)
    reference_frame_basis = jnp.linalg.qr(jax.random.normal(random_subkeys[0], (CELL_COMPONENTS, CELL_COMPONENTS), jnp.float32))[0]
    slow_count = CELL_COMPONENTS // 2
    shuffled = jax.random.permutation(random_subkeys[1], CELL_COMPONENTS)
    slow_row_mask = shuffled < slow_count
    same_group = (slow_row_mask[:, None] == slow_row_mask[None, :]).astype(jnp.float32)
    group_weight = same_group + 0.03 * (1.0 - same_group)
    mixing = jax.random.normal(random_subkeys[2], (TOTAL_BLOCK_ROWS, CELL_COMPONENTS, CELL_COMPONENTS), jnp.float32) * group_weight
    rotation = jnp.linalg.qr(mixing)[0]
    fast_rate = jnp.exp(jax.random.uniform(random_subkeys[3], (CELL_COMPONENTS,), jnp.float32, math.log(0.0005), math.log(0.2)))
    slow_rate = math.log(10.0) / (4.0 * TOTAL_BLOCK_ROWS)
    base_rate = jnp.where(slow_row_mask, slow_rate, fast_rate)
    diagonal_nudge = jnp.exp(jax.random.uniform(random_subkeys[4], (TOTAL_BLOCK_ROWS, CELL_COMPONENTS), jnp.float32, math.log(0.5), math.log(2.0)))
    damping_multiplier = jnp.exp(-base_rate[None, :] * diagonal_nudge)
    spike_row_indices = jax.random.randint(random_subkeys[5], (3,), 0, TOTAL_BLOCK_ROWS)
    spike_row_mask = jnp.any(jnp.arange(TOTAL_BLOCK_ROWS)[:, None] == spike_row_indices[None, :], axis=1)
    spike_keep_flags = jax.random.uniform(random_subkeys[6], (TOTAL_BLOCK_ROWS, CELL_COMPONENTS), jnp.float32, 0.5, 0.8)
    damping_multiplier = damping_multiplier * jnp.where(spike_row_mask[:, None] & slow_row_mask[None, :], spike_keep_flags, 1.0)
    scaled_result = damping_multiplier[:, :, None] * rotation
    return jnp.einsum('jr,erf,lf->ejl', reference_frame_basis, scaled_result, reference_frame_basis, precision=EXACT_ARITHMETIC)


def draw_upper_unit(key, part):
    return chain_factors(key, 11)


def draw_lower_unit(key, part):
    return chain_factors(key, 23)


def draw_pivot_inv(key, part):
    salted = jax.random.fold_in(key, 37)
    random_subkeys = jax.random.split(salted, 2)
    diagonal = jnp.exp(jax.random.uniform(random_subkeys[0], (TOTAL_BLOCK_ROWS, CELL_COMPONENTS), jnp.float32, math.log(0.5), math.log(2.0)))
    perturb = jnp.clip(jax.random.normal(random_subkeys[1], (TOTAL_BLOCK_ROWS, CELL_COMPONENTS, CELL_COMPONENTS), jnp.float32), -4.0, 4.0)
    perturb = perturb * (0.3 / math.sqrt(CELL_COMPONENTS))
    return perturb + diagonal[:, :, None] * jnp.eye(CELL_COMPONENTS, dtype=jnp.float32)


def block_scale(stream_key, shape, cuts, low, high):
    def one(dim, parts):
        draws = jax.random.uniform(jax.random.fold_in(jax.random.fold_in(stream_key, 6), dim), (parts,), jnp.float32, low / len(cuts), high / len(cuts))
        return jnp.repeat(jnp.exp(draws), shape[dim] // parts).reshape((-1,) + (1,) * (len(shape) - dim - 1))

    factor_of = one(*cuts[0])
    for cut in cuts[1:]:
        factor_of = factor_of * one(*cut)
    return factor_of


def gaussian(key, shape, spread, limit, cuts=(), kind=jnp.bfloat16):
    values = jax.random.normal(key, shape, jnp.float32) * spread
    if len(cuts) > 0:
        values = block_scale(key, shape, cuts, -0.22, 0.18) * values
    return jnp.clip(values, min=-limit, max=limit).astype(kind)


def setup_inputs(seed: int = 0) -> dict:
    arg_keys = jax.random.split(jax.random.key(seed), 8)
    return {
        "upper_unit": draw_upper_unit(jax.random.fold_in(arg_keys[7], 71), 0),
        "lower_unit": draw_lower_unit(jax.random.fold_in(arg_keys[7], 71), 0),
        "pivot_inv": draw_pivot_inv(jax.random.fold_in(arg_keys[7], 71), 0),
        "loss_grad_one": gaussian(arg_keys[3], (TOTAL_BLOCK_ROWS, DIRECTIONS, CELL_COMPONENTS), 1.0, 6.0, ((0, 8), (1, 4)), jnp.float32),
        "loss_grad_two": gaussian(arg_keys[4], (TOTAL_BLOCK_ROWS, DIRECTIONS, CELL_COMPONENTS), (1.5 / TOTAL_BLOCK_ROWS), 0.1875, ((0, 8), (1, 4)), jnp.float32),
        "state_one": gaussian(arg_keys[5], (TOTAL_BLOCK_ROWS, DIRECTIONS, CELL_COMPONENTS), (0.1 / TOTAL_BLOCK_ROWS), 0.01171875, ((0, 8), (1, 4)), jnp.float32),
        "state_two": gaussian(arg_keys[6], (TOTAL_BLOCK_ROWS, DIRECTIONS, CELL_COMPONENTS), 0.1, 1.5, ((0, 8), (1, 4)), jnp.float32),
    }


EXACT_ARITHMETIC = lax.Precision.HIGHEST

def advance(carried, element):
    source_row, factor = element
    solved = source_row - carried
    return (jnp.dot(solved, factor, precision=EXACT_ARITHMETIC), solved)

def transposed_solve(right_side, upper_unit, lower_unit, pivot_inv):
    initial = jnp.zeros(right_side.shape[1:], jnp.float32)
    _, lifted = lax.scan(advance, initial, (right_side, upper_unit))
    scaled_result = jnp.einsum('irb,ibc->irc', lifted, pivot_inv, precision=EXACT_ARITHMETIC)
    _, result = lax.scan(advance, initial, (scaled_result, lower_unit), reverse=True)
    return result

def outer_sum(adjoint, stored):
    return jnp.einsum('ira,irb->aib', adjoint, stored, precision=EXACT_ARITHMETIC)

def reference(upper_unit, lower_unit, pivot_inv, loss_grad_one, loss_grad_two, state_one, state_two):
    adjoint_two = transposed_solve(loss_grad_two, upper_unit, lower_unit, pivot_inv)
    adjoint_one = transposed_solve(loss_grad_one + adjoint_two, upper_unit, lower_unit, pivot_inv)
    zero_row = jnp.zeros_like(state_one[:1])
    variants = ((state_one, state_two), (jnp.concatenate([zero_row, state_one[:-1]], axis=0), jnp.concatenate([zero_row, state_two[:-1]], axis=0)), (jnp.concatenate([state_one[1:], zero_row], axis=0), jnp.concatenate([state_two[1:], zero_row], axis=0)))
    pieces = []
    for solution_past_opening, solution_past_closing in variants:
        pieces.append(outer_sum(adjoint_one, solution_past_opening) + outer_sum(adjoint_two, solution_past_closing))
    return -jnp.stack(pieces, axis=1)
```

```python
import functools

import jax
import jax.numpy as jnp
from jax import lax
from jax.experimental import pallas as pl
from jax.experimental.pallas import tpu as pltpu
from jax.sharding import PartitionSpec as P

MESH = pl.DeviceIdType.MESH
F32 = jnp.float32
BF16 = jnp.bfloat16


def halves(x):
    high = x.astype(BF16)
    return high, (x - high.astype(F32)).astype(BF16)


def tall(x):
    return jnp.concatenate(halves(x), axis=0)


def wide(x):
    return jnp.concatenate(halves(x), axis=1)


def product(left, right):
    r = jnp.dot(left, right, preferred_element_type=F32)
    m, n = r.shape[0] // 2, r.shape[1] // 2
    return r[:m, :n] + (r[:m, n:] + r[m:, :n])


def kernel(
    n, nq,
    upper, lower, pivot, grad_one, grad_two, state_one, state_two,
    out,
    acat, pcat, scat, vcat, wcat, mine, maps, ends, arrive, gcat, work, solved,
    packed, shares, states, lhs,
    m_send, m_recv, p_send, p_recv, a_send, a_recv, s_send, s_recv, h_send, h_recv, l_sem,
):
    rows, dirs, width = grad_one.shape
    d = lax.axis_index("rows")
    q = lax.axis_index("rhs")
    cut = width // nq
    groups = rows // nq
    own_states = (state_one, state_two)

    def at(i, size):
        return pl.ds(pl.multiple_of(i * size, size), size)

    def target(direction, k):
        return d + 1 + k if direction == 0 else d - 1 - k

    def sends(direction, k):
        return d + 1 + k < n if direction == 0 else d - 1 - k >= 0

    def gets(direction, k):
        return sends(1 - direction, k)

    def map_copy(direction, k):
        return pltpu.make_async_remote_copy(
            src_ref=mine.at[direction], dst_ref=maps.at[direction, k],
            send_sem=m_send.at[direction, k], recv_sem=m_recv.at[direction, k],
            device_id={"rows": target(direction, k)}, device_id_type=MESH)

    def end_copy(sweep, k):
        return pltpu.make_async_remote_copy(
            src_ref=ends.at[sweep], dst_ref=arrive.at[sweep, k],
            send_sem=p_send.at[sweep, k], recv_sem=p_recv.at[sweep, k],
            device_id={"rows": target(sweep % 2, k)}, device_id_type=MESH)

    def share_copy(which, t, src, dst):
        return pltpu.make_async_remote_copy(
            src_ref=packed.at[which, dst], dst_ref=shares.at[:, which, src],
            send_sem=a_send.at[which, t], recv_sem=a_recv.at[which, t],
            device_id={"rhs": dst}, device_id_type=MESH)

    def state_copy(which, t, src, dst):
        return pltpu.make_async_remote_copy(
            src_ref=own_states[which], dst_ref=states.at[pl.ds(1, rows), which, src],
            send_sem=s_send.at[which, t], recv_sem=s_recv.at[which, t],
            device_id={"rhs": dst}, device_id_type=MESH)

    def halo_copy(direction, which, t, src, dst):
        row, slot = (rows - 1, 0) if direction == 0 else (0, rows + 1)
        return pltpu.make_async_remote_copy(
            src_ref=own_states[which].at[row], dst_ref=states.at[slot, which, src],
            send_sem=h_send.at[direction, which, t], recv_sem=h_recv.at[direction, which, t],
            device_id={"rows": target(direction, 0), "rhs": dst}, device_id_type=MESH)

    def ahead(t):
        return lax.rem(q + t, nq)

    def behind(t):
        return lax.rem(q + nq - t, nq)

    for which in range(2):
        for t in range(1, nq):
            state_copy(which, t - 1, q, ahead(t)).start()
    local = [
        pltpu.make_async_copy(
            own_states[which], states.at[pl.ds(1, rows), which, q], l_sem.at[which])
        for which in range(2)
    ]
    for copy in local:
        copy.start()

    ones = (upper, lower)

    def prepare(i, _):
        vcat[i] = wide(pivot[i])
        for side in range(2):
            acat[side, i] = wide(-ones[side][i])
        gcat[:, at(i, width)] = tall(grad_two[i])
        return 0

    lax.fori_loop(0, rows, prepare, 0)

    last = rows - 1
    for side in range(2):
        first, final = (0, last) if side == 0 else (last, 0)
        pcat[side, :, first * 2 * width:(first + 1) * 2 * width] = acat[side, first]
        scat[side, final * width:(final + 1) * width, :] = acat[side, final]

    def stack(high_low):
        return jnp.concatenate([high_low[:, :width], high_low[:, width:]], axis=0)

    def grow(step, _):
        for side in range(2):
            if side == 0:
                i, prev, j, after = step, step - 1, last - step, last - step + 1
            else:
                i, prev, j, after = last - step, last - step + 1, step, step - 1
            before = stack(pcat[side, :, at(prev, 2 * width)])
            pcat[side, :, at(i, 2 * width)] = wide(product(before, acat[side, i]))
            suffix = product(stack(acat[side, j]), scat[side, at(after, width), :])
            scat[side, at(j, width), :] = wide(suffix)
            mine[side] = suffix
        return 0

    lax.fori_loop(1, rows, grow, 0)

    for k in range(n - 2):
        for direction in range(2):
            @pl.when(sends(direction, k))
            def _():
                map_copy(direction, k).start()

    def send_end(sweep):
        ends[sweep] = -product(gcat[...], scat[sweep % 2])
        for k in range(n - 1):
            @pl.when(sends(sweep % 2, k))
            def _():
                end_copy(sweep, k).start()

    def chain(side, source):
        def link(step, carry):
            i = step if side == 0 else last - step
            y = source[i] + carry
            work[i] = y
            return product(tall(y), acat[side, i])

        lax.fori_loop(0, rows, link, jnp.zeros((dirs, width), F32))

    def relay(direction):
        def one(k, _):
            @pl.when(gets(direction, k))
            def _():
                map_copy(direction, k).wait_recv()

            @pl.when(jnp.logical_not(gets(direction, k)))
            def _():
                maps[direction, k] = jnp.zeros((width, width), F32)

            @pl.when(k == 0)
            def _():
                wcat[direction, 0:width, :] = wide(maps[direction, 0])

            @pl.when(k > 0)
            def _():
                wcat[direction, at(k, width), :] = wide(
                    product(tall(maps[direction, k]), wcat[direction, at(lax.max(k - 1, 0), width), :]))
            return 0

        lax.fori_loop(0, n - 2, one, 0)

    def incoming(sweep):
        for k in range(n - 1):
            @pl.when(gets(sweep % 2, k))
            def _():
                end_copy(sweep, k).wait_recv()

            @pl.when(jnp.logical_not(gets(sweep % 2, k)))
            def _():
                arrive[sweep, k] = jnp.zeros((dirs, width), F32)
        total = arrive[sweep, 0]
        if n > 2:
            rest = jnp.concatenate([arrive[sweep, k] for k in range(1, n - 1)], axis=1)
            total = total + product(tall(rest), wcat[sweep % 2])
        return total

    def spread(side, carry):
        r = jnp.dot(tall(carry), pcat[side], preferred_element_type=F32)
        parts = []
        for i in range(rows):
            c = i * 2 * width
            parts.append(r[:dirs, c:c + width]
                         + (r[:dirs, c + width:c + 2 * width] + r[dirs:, c:c + width]))
        return parts

    def solve(first_sweep, source, between):
        send_end(first_sweep)
        between()
        chain(0, source)
        if first_sweep == 0:
            relay(0)
        carry = incoming(first_sweep)
        parts = [carry] + spread(0, carry)[:-1]
        for i in range(rows):
            z = product(tall(work[i] - parts[i]), vcat[i])
            solved[i] = z
            gcat[:, i * width:(i + 1) * width] = tall(z)
        send_end(first_sweep + 1)
        chain(1, solved)
        if first_sweep == 0:
            relay(1)
        carry = incoming(first_sweep + 1)
        parts = spread(1, carry)[1:] + [carry]
        return [work[i] - parts[i] for i in range(rows)]

    def start_halo():
        for direction in range(2):
            @pl.when(sends(direction, 0))
            def _():
                for which in range(2):
                    for t in range(nq):
                        halo_copy(direction, which, t, q, ahead(t)).start()

    lane = lax.broadcasted_iota(jnp.int32, (dirs, width), 1)

    def share(which, adjoint):
        for g in range(groups):
            for dst in range(nq):
                piece = None
                for ii in range(nq):
                    shift = ((ii - dst) * cut) % width
                    x = adjoint[g * nq + ii]
                    x = pltpu.roll(x, shift, 1) if shift else x
                    piece = x if piece is None else jnp.where(lane >= ii * cut, x, piece)
                packed[which, dst, g] = piece
        for t in range(1, nq):
            share_copy(which, t - 1, q, ahead(t)).start()
        copy = pltpu.make_async_copy(
            packed.at[which, q], shares.at[:, which, q], l_sem.at[2 + which])
        copy.start()
        local.append(copy)

    adjoint_two = solve(0, grad_two, start_halo)
    for i in range(rows):
        total = grad_one[i] + adjoint_two[i]
        solved[i] = total
        gcat[:, i * width:(i + 1) * width] = tall(total)
    adjoint_one = solve(2, solved, lambda: share(1, adjoint_two))
    share(0, adjoint_one)

    for which in range(2):
        for t in range(1, nq):
            state_copy(which, t - 1, behind(t), q).wait_recv()
    for direction in range(2):
        @pl.when(gets(direction, 0))
        def _():
            for which in range(2):
                for t in range(nq):
                    halo_copy(direction, which, t, behind(t), q).wait_recv()

        @pl.when(jnp.logical_not(gets(direction, 0)))
        def _():
            slot = 0 if direction == 0 else rows + 1
            states[slot] = jnp.zeros(states.shape[1:], F32)
    for which in (1, 0):
        for t in range(1, nq):
            share_copy(which, t - 1, behind(t), q).wait_recv()
    for copy in local:
        copy.wait()

    depth = 2 * nq * dirs
    for g in range(groups):
        turned = jnp.transpose(shares[g].reshape(depth, width))
        high, low = halves(turned)
        lhs[0, g * width:(g + 1) * width, :] = high
        lhs[1, g * width:(g + 1) * width, :] = low
    for j in range(rows + 2):
        low_row, high_row = max(j - 2, 0), min(j, last)
        a, b = low_row * cut, (high_row + 1) * cut
        left = jnp.concatenate([lhs[0, a:b, :], lhs[1, a:b, :]], axis=0)
        r = product(left, wide(states[j].reshape(depth, width)))
        for i in range(low_row, high_row + 1):
            piece = {j - 1: 0, j: 1, j - 2: 2}[i]
            out[i, piece] = -r[(i - low_row) * cut:(i - low_row + 1) * cut, :]

    for which in range(2):
        for t in range(1, nq):
            state_copy(which, t - 1, q, ahead(t)).wait_send()
            share_copy(which, t - 1, q, ahead(t)).wait_send()
    for direction in range(2):
        @pl.when(sends(direction, 0))
        def _():
            for which in range(2):
                for t in range(nq):
                    halo_copy(direction, which, t, q, ahead(t)).wait_send()

        for k in range(n - 2):
            @pl.when(sends(direction, k))
            def _():
                map_copy(direction, k).wait_send()
    for sweep in range(4):
        for k in range(n - 1):
            @pl.when(sends(sweep % 2, k))
            def _():
                end_copy(sweep, k).wait_send()


def body(n, nq, *args):
    rows, dirs, width = args[3].shape
    cut = width // nq
    groups = rows // nq
    depth = 2 * nq * dirs
    dma = pltpu.SemaphoreType.DMA
    vmem = pl.BlockSpec(memory_space=pltpu.VMEM)
    result = pl.pallas_call(
        functools.partial(kernel, n, nq),
        out_shape=jax.ShapeDtypeStruct((rows, 3, cut, width), F32),
        in_specs=[vmem] * 7,
        out_specs=vmem,
        scratch_shapes=[
            pltpu.VMEM((2, rows, width, 2 * width), BF16),
            pltpu.VMEM((2, width, rows * 2 * width), BF16),
            pltpu.VMEM((2, rows * width, 2 * width), BF16),
            pltpu.VMEM((rows, width, 2 * width), BF16),
            pltpu.VMEM((2, (n - 2) * width, 2 * width), BF16),
            pltpu.VMEM((2, width, width), F32),
            pltpu.VMEM((2, n - 2, width, width), F32),
            pltpu.VMEM((4, dirs, width), F32),
            pltpu.VMEM((4, n - 1, dirs, width), F32),
            pltpu.VMEM((2 * dirs, rows * width), BF16),
            pltpu.VMEM((rows, dirs, width), F32),
            pltpu.VMEM((rows, dirs, width), F32),
            pltpu.VMEM((2, nq, groups, dirs, width), F32),
            pltpu.VMEM((groups, 2, nq, dirs, width), F32),
            pltpu.VMEM((rows + 2, 2, nq, dirs, width), F32),
            pltpu.VMEM((2, rows * cut, depth), BF16),
            dma((2, n - 2)), dma((2, n - 2)),
            dma((4, n - 1)), dma((4, n - 1)),
            dma((2, nq - 1)), dma((2, nq - 1)),
            dma((2, nq - 1)), dma((2, nq - 1)),
            dma((2, 2, nq)), dma((2, 2, nq)),
            dma((4,)),
        ],
        compiler_params=pltpu.CompilerParams(
            has_side_effects=True, vmem_limit_bytes=60 * 1024 * 1024),
    )(*args)
    return jnp.transpose(result, (2, 1, 0, 3))


def solution(mesh):
    factors = P("rows", None, None)
    vectors = P("rows", "rhs", None)
    return jax.shard_map(
        functools.partial(body, mesh.shape["rows"], mesh.shape["rhs"]),
        mesh=mesh,
        in_specs=(factors,) * 3 + (vectors,) * 4,
        out_specs=P("rhs", None, "rows", None),
        check_vma=False,
    )
```

```python
import functools

import jax
import jax.numpy as jnp
from jax import lax
from jax.experimental import pallas as pl
from jax.experimental.pallas import tpu as pltpu
from jax.sharding import PartitionSpec as P

MESH = pl.DeviceIdType.MESH
F32 = jnp.float32
BF16 = jnp.bfloat16


def halves(x):
    high = x.astype(BF16)
    return high, (x - high.astype(F32)).astype(BF16)


def tall(x):
    return jnp.concatenate(halves(x), axis=0)


def wide(x):
    return jnp.concatenate(halves(x), axis=1)


def product(left, right):
    r = jnp.dot(left, right, preferred_element_type=F32)
    m, n = r.shape[0] // 2, r.shape[1] // 2
    return r[:m, :n] + (r[:m, n:] + r[m:, :n])


def kernel(
    n, nq,
    upper, lower, pivot, grad_one, grad_two, state_one, state_two,
    out,
    acat, tree, pcat, scat, vcat, wcat, mine, maps, ends, arrive, gcat, work, solved,
    packed, shares, states, lhs,
    m_send, m_recv, f_send, f_recv, p_send, p_recv, a_send, a_recv, s_send, s_recv, t_send, t_recv, h_send, h_recv, l_sem,
):
    rows, dirs, width = grad_one.shape
    d = lax.axis_index("rows")
    q = lax.axis_index("rhs")
    cut = width // nq
    groups = rows // nq
    own_states = (state_one, state_two)

    def at(i, size):
        return pl.ds(pl.multiple_of(i * size, size), size)

    def target(direction, k):
        return d + 1 + k if direction == 0 else d - 1 - k

    def sends(direction, k):
        return d + 1 + k < n if direction == 0 else d - 1 - k >= 0

    def gets(direction, k):
        return sends(1 - direction, k)

    half = width // 2
    parity = lax.rem(q, 2)
    partner = q + 1 - 2 * parity
    pairs = nq // 2

    def map_copy(direction, k):
        part = at(parity, half)
        return pltpu.make_async_remote_copy(
            src_ref=mine.at[direction, part], dst_ref=maps.at[direction, k, part],
            send_sem=m_send.at[direction, k], recv_sem=m_recv.at[direction, k],
            device_id={"rows": target(direction, k)}, device_id_type=MESH)

    def map_forward(direction, k, owner):
        part = at(owner, half)
        return pltpu.make_async_remote_copy(
            src_ref=maps.at[direction, k, part], dst_ref=maps.at[direction, k, part],
            send_sem=f_send.at[direction, k], recv_sem=f_recv.at[direction, k],
            device_id={"rhs": partner}, device_id_type=MESH)

    def end_copy(sweep, k):
        return pltpu.make_async_remote_copy(
            src_ref=ends.at[sweep], dst_ref=arrive.at[sweep, k],
            send_sem=p_send.at[sweep, k], recv_sem=p_recv.at[sweep, k],
            device_id={"rows": target(sweep % 2, k)}, device_id_type=MESH)

    def share_copy(which, t, src, dst):
        return pltpu.make_async_remote_copy(
            src_ref=packed.at[which, dst], dst_ref=shares.at[:, which, src],
            send_sem=a_send.at[which, t], recv_sem=a_recv.at[which, t],
            device_id={"rhs": dst}, device_id_type=MESH)

    def state_copy(which, t, src, dst):
        return pltpu.make_async_remote_copy(
            src_ref=own_states[which], dst_ref=states.at[pl.ds(1, rows), which, src],
            send_sem=s_send.at[which, t], recv_sem=s_recv.at[which, t],
            device_id={"rhs": dst}, device_id_type=MESH)

    def state_forward(which, t, src):
        block = states.at[pl.ds(1, rows), which, src]
        return pltpu.make_async_remote_copy(
            src_ref=own_states[which] if t == 0 else block, dst_ref=block,
            send_sem=t_send.at[which, t], recv_sem=t_recv.at[which, t],
            device_id={"rhs": partner}, device_id_type=MESH)

    def halo_copy(direction, which, t, src, dst):
        row, slot = (rows - 1, 0) if direction == 0 else (0, rows + 1)
        return pltpu.make_async_remote_copy(
            src_ref=own_states[which].at[row], dst_ref=states.at[slot, which, src],
            send_sem=h_send.at[direction, which, t], recv_sem=h_recv.at[direction, which, t],
            device_id={"rows": target(direction, 0), "rhs": dst}, device_id_type=MESH)

    def ahead(t):
        return lax.rem(q + t, nq)

    def behind(t):
        return lax.rem(q + nq - t, nq)

    barrier = pltpu.get_barrier_semaphore()
    met = [{"rows": lax.rem(d + t, n)} for t in range(1, n)]
    met += [{"rhs": ahead(t)} for t in range(1, nq)]
    met += [{"rows": lax.rem(d + s, n), "rhs": ahead(t)} for s in (1, n - 1) for t in range(1, nq)]
    for other in met:
        pl.semaphore_signal(barrier, inc=1, device_id=other, device_id_type=MESH)

    local = [
        pltpu.make_async_copy(
            own_states[which], states.at[pl.ds(1, rows), which, q], l_sem.at[which])
        for which in range(2)
    ]
    for copy in local:
        copy.start()

    ones = (upper, lower)

    def prepare(i, _):
        vcat[i] = wide(pivot[i])
        for side in range(2):
            acat[side, i] = wide(-ones[side][i])
        gcat[:, at(i, width)] = tall(grad_two[i])
        return 0

    lax.fori_loop(0, rows, prepare, 0)

    last = rows - 1

    def stack(high_low):
        return jnp.concatenate([high_low[:, :width], high_low[:, width:]], axis=0)

    def row_of(side, m):
        return m if side == 0 else last - m

    def branch(side, start, size):
        if size == 1:
            return acat[side, row_of(side, start)]
        return tree[side, rows - 2 * rows // size + start // size]

    size = 2
    while size <= rows:
        for start in range(0, rows, size):
            for side in range(2):
                value = product(
                    stack(branch(side, start, size // 2)), branch(side, start + size // 2, size // 2))
                tree[side, rows - 2 * rows // size + start // size] = wide(value)
                if size == rows:
                    mine[side] = value
        size *= 2

    pl.semaphore_wait(barrier, len(met))
    for k in range(n - 2):
        for direction in range(2):
            @pl.when(sends(direction, k))
            def _():
                map_copy(direction, k).start()
    for which in range(2):
        for t in range(1, pairs):
            state_copy(which, t - 1, q, ahead(2 * t)).start()
        state_forward(which, 0, q).start()

    def prefix_at(side, count):
        i = row_of(side, count - 1)
        return slice(i * 2 * width, (i + 1) * 2 * width)

    def suffix_at(side, count):
        i = row_of(side, rows - count)
        return slice(i * width, (i + 1) * width)

    low = rows
    while low >= 1:
        for count in range(low, rows + 1, 2 * low):
            for side in range(2):
                start = rows - count
                if count == low:
                    pcat[side, :, prefix_at(side, count)] = branch(side, 0, low)
                    scat[side, suffix_at(side, count), :] = branch(side, start, low)
                else:
                    before = pcat[side, :, prefix_at(side, count - low)]
                    pcat[side, :, prefix_at(side, count)] = wide(
                        product(stack(before), branch(side, count - low, low)))
                    after = scat[side, suffix_at(side, count - low), :]
                    scat[side, suffix_at(side, count), :] = wide(
                        product(stack(branch(side, start, low)), after))
        low //= 2

    def send_end(sweep):
        ends[sweep] = -product(gcat[...], scat[sweep % 2])
        for k in range(n - 1):
            @pl.when(sends(sweep % 2, k))
            def _():
                end_copy(sweep, k).start()

    def chain(side, source):
        def link(step, carry):
            i = step if side == 0 else last - step
            y = source[i] + carry
            work[i] = y
            return product(tall(y), acat[side, i])

        lax.fori_loop(0, rows, link, jnp.zeros((dirs, width), F32))

    def relay(direction):
        def one(k, _):
            @pl.when(gets(direction, k))
            def _():
                map_forward(direction, k, 1 - parity).wait_recv()

            @pl.when(jnp.logical_not(gets(direction, k)))
            def _():
                maps[direction, k] = jnp.zeros((width, width), F32)

            @pl.when(k == 0)
            def _():
                wcat[direction, 0:width, :] = wide(maps[direction, 0])

            @pl.when(k > 0)
            def _():
                wcat[direction, at(k, width), :] = wide(
                    product(tall(maps[direction, k]), wcat[direction, at(lax.max(k - 1, 0), width), :]))
            return 0

        lax.fori_loop(0, n - 2, one, 0)

    def incoming(sweep):
        for k in range(n - 1):
            @pl.when(gets(sweep % 2, k))
            def _():
                end_copy(sweep, k).wait_recv()

            @pl.when(jnp.logical_not(gets(sweep % 2, k)))
            def _():
                arrive[sweep, k] = jnp.zeros((dirs, width), F32)
        total = arrive[sweep, 0]
        if n > 2:
            rest = jnp.concatenate([arrive[sweep, k] for k in range(1, n - 1)], axis=1)
            total = total + product(tall(rest), wcat[sweep % 2])
        return total

    def spread(side, carry):
        r = jnp.dot(tall(carry), pcat[side], preferred_element_type=F32)
        parts = []
        for i in range(rows):
            c = i * 2 * width
            parts.append(r[:dirs, c:c + width]
                         + (r[:dirs, c + width:c + 2 * width] + r[dirs:, c:c + width]))
        return parts

    def solve(first_sweep, source, between):
        send_end(first_sweep)
        between()
        chain(0, source)
        if first_sweep == 0:
            for direction in range(2):
                for k in range(n - 2):
                    @pl.when(gets(direction, k))
                    def _():
                        map_copy(direction, k).wait_recv()
                        map_forward(direction, k, parity).start()
            relay(0)
        carry = incoming(first_sweep)
        parts = [carry] + spread(0, carry)[:-1]
        for i in range(rows):
            z = product(tall(work[i] - parts[i]), vcat[i])
            solved[i] = z
            gcat[:, i * width:(i + 1) * width] = tall(z)
        send_end(first_sweep + 1)
        chain(1, solved)
        if first_sweep == 0:
            relay(1)
        carry = incoming(first_sweep + 1)
        parts = spread(1, carry)[1:] + [carry]
        return [work[i] - parts[i] for i in range(rows)]

    def start_halo():
        for direction in range(2):
            @pl.when(sends(direction, 0))
            def _():
                for which in range(2):
                    for t in range(nq):
                        halo_copy(direction, which, t, q, ahead(t)).start()

    lane = lax.broadcasted_iota(jnp.int32, (dirs, width), 1)

    def share(which, adjoint):
        for g in range(groups):
            for dst in range(nq):
                piece = None
                for ii in range(nq):
                    shift = ((ii - dst) * cut) % width
                    x = adjoint[g * nq + ii]
                    x = pltpu.roll(x, shift, 1) if shift else x
                    piece = x if piece is None else jnp.where(lane >= ii * cut, x, piece)
                packed[which, dst, g] = piece
        for t in range(1, nq):
            share_copy(which, t - 1, q, ahead(t)).start()
        copy = pltpu.make_async_copy(
            packed.at[which, q], shares.at[:, which, q], l_sem.at[2 + which])
        copy.start()
        local.append(copy)

    adjoint_two = solve(0, grad_two, start_halo)
    for i in range(rows):
        total = grad_one[i] + adjoint_two[i]
        solved[i] = total
        gcat[:, i * width:(i + 1) * width] = tall(total)
    def pass_on():
        share(1, adjoint_two)
        for which in range(2):
            for t in range(1, pairs):
                state_copy(which, t - 1, behind(2 * t), q).wait_recv()
                state_forward(which, t, behind(2 * t)).start()

    adjoint_one = solve(2, solved, pass_on)
    share(0, adjoint_one)

    for which in range(2):
        for t in range(pairs):
            state_forward(which, t, lax.rem(partner + nq - 2 * t, nq)).wait_recv()
    for direction in range(2):
        @pl.when(gets(direction, 0))
        def _():
            for which in range(2):
                for t in range(nq):
                    halo_copy(direction, which, t, behind(t), q).wait_recv()

        @pl.when(jnp.logical_not(gets(direction, 0)))
        def _():
            slot = 0 if direction == 0 else rows + 1
            states[slot] = jnp.zeros(states.shape[1:], F32)
    for which in (1, 0):
        for t in range(1, nq):
            share_copy(which, t - 1, behind(t), q).wait_recv()
    for copy in local:
        copy.wait()

    depth = 2 * nq * dirs
    for g in range(groups):
        turned = jnp.transpose(shares[g].reshape(depth, width))
        high, low = halves(turned)
        lhs[0, g * width:(g + 1) * width, :] = high
        lhs[1, g * width:(g + 1) * width, :] = low
    for j in range(rows + 2):
        low_row, high_row = max(j - 2, 0), min(j, last)
        a, b = low_row * cut, (high_row + 1) * cut
        left = jnp.concatenate([lhs[0, a:b, :], lhs[1, a:b, :]], axis=0)
        r = product(left, wide(states[j].reshape(depth, width)))
        for i in range(low_row, high_row + 1):
            piece = {j - 1: 0, j: 1, j - 2: 2}[i]
            out[pl.ds(piece * rows + i, cut, stride=3 * rows), :] = (
                -r[(i - low_row) * cut:(i - low_row + 1) * cut, :])

    for which in range(2):
        for t in range(1, pairs):
            state_copy(which, t - 1, q, ahead(2 * t)).wait_send()
        for t in range(pairs):
            state_forward(which, t, behind(2 * t)).wait_send()
        for t in range(1, nq):
            share_copy(which, t - 1, q, ahead(t)).wait_send()
    for direction in range(2):
        @pl.when(sends(direction, 0))
        def _():
            for which in range(2):
                for t in range(nq):
                    halo_copy(direction, which, t, q, ahead(t)).wait_send()

        for k in range(n - 2):
            @pl.when(sends(direction, k))
            def _():
                map_copy(direction, k).wait_send()

            @pl.when(gets(direction, k))
            def _():
                map_forward(direction, k, parity).wait_send()
    for sweep in range(4):
        for k in range(n - 1):
            @pl.when(sends(sweep % 2, k))
            def _():
                end_copy(sweep, k).wait_send()


def body(n, nq, *args):
    rows, dirs, width = args[3].shape
    cut = width // nq
    groups = rows // nq
    depth = 2 * nq * dirs
    dma = pltpu.SemaphoreType.DMA
    vmem = pl.BlockSpec(memory_space=pltpu.VMEM)
    result = pl.pallas_call(
        functools.partial(kernel, n, nq),
        out_shape=jax.ShapeDtypeStruct((cut * 3 * rows, width), F32),
        in_specs=[vmem] * 7,
        out_specs=vmem,
        scratch_shapes=[
            pltpu.VMEM((2, rows, width, 2 * width), BF16),
            pltpu.VMEM((2, rows - 1, width, 2 * width), BF16),
            pltpu.VMEM((2, width, rows * 2 * width), BF16),
            pltpu.VMEM((2, rows * width, 2 * width), BF16),
            pltpu.VMEM((rows, width, 2 * width), BF16),
            pltpu.VMEM((2, (n - 2) * width, 2 * width), BF16),
            pltpu.VMEM((2, width, width), F32),
            pltpu.VMEM((2, n - 2, width, width), F32),
            pltpu.VMEM((4, dirs, width), F32),
            pltpu.VMEM((4, n - 1, dirs, width), F32),
            pltpu.VMEM((2 * dirs, rows * width), BF16),
            pltpu.VMEM((rows, dirs, width), F32),
            pltpu.VMEM((rows, dirs, width), F32),
            pltpu.VMEM((2, nq, groups, dirs, width), F32),
            pltpu.VMEM((groups, 2, nq, dirs, width), F32),
            pltpu.VMEM((rows + 2, 2, nq, dirs, width), F32),
            pltpu.VMEM((2, rows * cut, depth), BF16),
            dma((2, n - 2)), dma((2, n - 2)),
            dma((2, n - 2)), dma((2, n - 2)),
            dma((4, n - 1)), dma((4, n - 1)),
            dma((2, nq - 1)), dma((2, nq - 1)),
            dma((2, max(nq // 2 - 1, 1))), dma((2, max(nq // 2 - 1, 1))),
            dma((2, nq // 2)), dma((2, nq // 2)),
            dma((2, 2, nq)), dma((2, 2, nq)),
            dma((4,)),
        ],
        compiler_params=pltpu.CompilerParams(
            collective_id=0, has_side_effects=True, vmem_limit_bytes=60 * 1024 * 1024),
    )(*args)
    return result.reshape(cut, 3, rows, width)


def solution(mesh):
    factors = P("rows", None, None)
    vectors = P("rows", "rhs", None)
    return jax.shard_map(
        functools.partial(body, mesh.shape["rows"], mesh.shape["rhs"]),
        mesh=mesh,
        in_specs=(factors,) * 3 + (vectors,) * 4,
        out_specs=P("rhs", None, "rows", None),
        check_vma=False,
    )
```

```python
import functools

import jax
import jax.numpy as jnp
from jax import lax
from jax.experimental import pallas as pl
from jax.experimental.pallas import tpu as pltpu
from jax.sharding import PartitionSpec as P

MESH = pl.DeviceIdType.MESH
F32 = jnp.float32
BF16 = jnp.bfloat16


def halves(x):
    high = x.astype(BF16)
    return high, (x - high.astype(F32)).astype(BF16)


def tall(x):
    return jnp.concatenate(halves(x), axis=0)


def wide(x):
    return jnp.concatenate(halves(x), axis=1)


def product(left, right):
    r = jnp.dot(left, right, preferred_element_type=F32)
    m, n = r.shape[0] // 2, r.shape[1] // 2
    return r[:m, :n] + (r[:m, n:] + r[m:, :n])


def kernel(
    n, nq,
    upper, lower, pivot, grad_one, grad_two, state_one, state_two,
    out,
    acat, tree, pcat, scat, vcat, wcat, mine, maps, ends, arrive, gcat, work, solved,
    packed, shares, states, lhs,
    m_send, m_recv, f_send, f_recv, p_send, p_recv, a_send, a_recv, s_send, s_recv, t_send, t_recv, h_send, h_recv, l_sem,
):
    rows, dirs, width = grad_one.shape
    d = lax.axis_index("rows")
    q = lax.axis_index("rhs")
    cut = width // nq
    groups = rows // nq
    own_states = (state_one, state_two)

    def at(i, size):
        return pl.ds(pl.multiple_of(i * size, size), size)

    def target(direction, k):
        return d + 1 + k if direction == 0 else d - 1 - k

    def sends(direction, k):
        return d + 1 + k < n if direction == 0 else d - 1 - k >= 0

    def gets(direction, k):
        return sends(1 - direction, k)

    half = width // 2
    parity = lax.rem(q, 2)
    partner = q + 1 - 2 * parity
    pairs = nq // 2

    def map_copy(direction, k):
        part = at(parity, half)
        return pltpu.make_async_remote_copy(
            src_ref=mine.at[direction, part], dst_ref=maps.at[direction, k, part],
            send_sem=m_send.at[direction, k], recv_sem=m_recv.at[direction, k],
            device_id={"rows": target(direction, k)}, device_id_type=MESH)

    def map_forward(direction, k, owner):
        part = at(owner, half)
        return pltpu.make_async_remote_copy(
            src_ref=maps.at[direction, k, part], dst_ref=maps.at[direction, k, part],
            send_sem=f_send.at[direction, k], recv_sem=f_recv.at[direction, k],
            device_id={"rhs": partner}, device_id_type=MESH)

    def end_copy(sweep, k):
        return pltpu.make_async_remote_copy(
            src_ref=ends.at[sweep], dst_ref=arrive.at[sweep, k],
            send_sem=p_send.at[sweep, k], recv_sem=p_recv.at[sweep, k],
            device_id={"rows": target(sweep % 2, k)}, device_id_type=MESH)

    def share_copy(which, t, src, dst):
        return pltpu.make_async_remote_copy(
            src_ref=packed.at[which, dst], dst_ref=shares.at[:, which, src],
            send_sem=a_send.at[which, t], recv_sem=a_recv.at[which, t],
            device_id={"rhs": dst}, device_id_type=MESH)

    def state_copy(which, t, src, dst):
        return pltpu.make_async_remote_copy(
            src_ref=own_states[which], dst_ref=states.at[pl.ds(1, rows), which, src],
            send_sem=s_send.at[which, t], recv_sem=s_recv.at[which, t],
            device_id={"rhs": dst}, device_id_type=MESH)

    def state_forward(which, t, src):
        block = states.at[pl.ds(1, rows), which, src]
        return pltpu.make_async_remote_copy(
            src_ref=own_states[which] if t == 0 else block, dst_ref=block,
            send_sem=t_send.at[which, t], recv_sem=t_recv.at[which, t],
            device_id={"rhs": partner}, device_id_type=MESH)

    def halo_copy(direction, which, t, src, dst):
        row, slot = (rows - 1, 0) if direction == 0 else (0, rows + 1)
        return pltpu.make_async_remote_copy(
            src_ref=own_states[which].at[row], dst_ref=states.at[slot, which, src],
            send_sem=h_send.at[direction, which, t], recv_sem=h_recv.at[direction, which, t],
            device_id={"rows": target(direction, 0), "rhs": dst}, device_id_type=MESH)

    def ahead(t):
        return lax.rem(q + t, nq)

    def behind(t):
        return lax.rem(q + nq - t, nq)

    barrier = pltpu.get_barrier_semaphore()
    met = [{"rows": lax.rem(d + t, n)} for t in range(1, n)]
    met += [{"rhs": ahead(t)} for t in range(1, nq)]
    met += [{"rows": lax.rem(d + s, n), "rhs": ahead(t)} for s in (1, n - 1) for t in range(1, nq)]
    for other in met:
        pl.semaphore_signal(barrier, inc=1, device_id=other, device_id_type=MESH)

    local = [
        pltpu.make_async_copy(
            own_states[which], states.at[pl.ds(1, rows), which, q], l_sem.at[which])
        for which in range(2)
    ]
    for copy in local:
        copy.start()

    ones = (upper, lower)

    def prepare(i, _):
        for side in range(2):
            acat[side, i] = wide(-ones[side][i])
        return 0

    def prepare_rest(i, _):
        vcat[i] = wide(pivot[i])
        gcat[:, at(i, width)] = tall(grad_two[i])
        return 0

    lax.fori_loop(0, rows, prepare, 0)

    last = rows - 1

    def stack(high_low):
        return jnp.concatenate([high_low[:, :width], high_low[:, width:]], axis=0)

    def row_of(side, m):
        return m if side == 0 else last - m

    def branch(side, start, size):
        if size == 1:
            return acat[side, row_of(side, start)]
        return tree[side, rows - 2 * rows // size + start // size]

    size = 2
    while size <= rows:
        for start in range(0, rows, size):
            for side in range(2):
                value = product(
                    stack(branch(side, start, size // 2)), branch(side, start + size // 2, size // 2))
                tree[side, rows - 2 * rows // size + start // size] = wide(value)
                if size == rows:
                    mine[side] = value
        size *= 2

    pl.semaphore_wait(barrier, len(met))
    for k in range(n - 2):
        for direction in range(2):
            @pl.when(sends(direction, k))
            def _():
                map_copy(direction, k).start()
    for which in range(2):
        for t in range(1, pairs):
            state_copy(which, t - 1, q, ahead(2 * t)).start()
        state_forward(which, 0, q).start()

    lax.fori_loop(0, rows, prepare_rest, 0)

    def prefix_at(side, count):
        i = row_of(side, count - 1)
        return slice(i * 2 * width, (i + 1) * 2 * width)

    def suffix_at(side, count):
        i = row_of(side, rows - count)
        return slice(i * width, (i + 1) * width)

    low = rows
    while low >= 1:
        for count in range(low, rows + 1, 2 * low):
            for side in range(2):
                start = rows - count
                if count == low:
                    pcat[side, :, prefix_at(side, count)] = branch(side, 0, low)
                    scat[side, suffix_at(side, count), :] = branch(side, start, low)
                else:
                    before = pcat[side, :, prefix_at(side, count - low)]
                    pcat[side, :, prefix_at(side, count)] = wide(
                        product(stack(before), branch(side, count - low, low)))
                    after = scat[side, suffix_at(side, count - low), :]
                    scat[side, suffix_at(side, count), :] = wide(
                        product(stack(branch(side, start, low)), after))
        low //= 2

    def send_end(sweep):
        ends[sweep] = -product(gcat[...], scat[sweep % 2])
        for k in range(n - 1):
            @pl.when(sends(sweep % 2, k))
            def _():
                end_copy(sweep, k).start()

    def chain(side, source):
        def link(step, carry):
            i = step if side == 0 else last - step
            y = source[i] + carry
            work[i] = y
            return product(tall(y), acat[side, i])

        lax.fori_loop(0, rows, link, jnp.zeros((dirs, width), F32))

    def relay(direction):
        def one(k, _):
            @pl.when(gets(direction, k))
            def _():
                map_forward(direction, k, 1 - parity).wait_recv()

            @pl.when(jnp.logical_not(gets(direction, k)))
            def _():
                maps[direction, k] = jnp.zeros((width, width), F32)

            @pl.when(k == 0)
            def _():
                wcat[direction, 0:width, :] = wide(maps[direction, 0])

            @pl.when(k > 0)
            def _():
                wcat[direction, at(k, width), :] = wide(
                    product(tall(maps[direction, k]), wcat[direction, at(lax.max(k - 1, 0), width), :]))
            return 0

        lax.fori_loop(0, n - 2, one, 0)

    def incoming(sweep):
        for k in range(n - 1):
            @pl.when(gets(sweep % 2, k))
            def _():
                end_copy(sweep, k).wait_recv()

            @pl.when(jnp.logical_not(gets(sweep % 2, k)))
            def _():
                arrive[sweep, k] = jnp.zeros((dirs, width), F32)
        total = arrive[sweep, 0]
        if n > 2:
            rest = jnp.concatenate([arrive[sweep, k] for k in range(1, n - 1)], axis=1)
            total = total + product(tall(rest), wcat[sweep % 2])
        return total

    def spread(side, carry):
        r = jnp.dot(tall(carry), pcat[side], preferred_element_type=F32)
        parts = []
        for i in range(rows):
            c = i * 2 * width
            parts.append(r[:dirs, c:c + width]
                         + (r[:dirs, c + width:c + 2 * width] + r[dirs:, c:c + width]))
        return parts

    def solve(first_sweep, source, between):
        send_end(first_sweep)
        between()
        chain(0, source)
        if first_sweep == 0:
            for direction in range(2):
                for k in range(n - 2):
                    @pl.when(gets(direction, k))
                    def _():
                        map_copy(direction, k).wait_recv()
                        map_forward(direction, k, parity).start()
            relay(0)
        carry = incoming(first_sweep)
        parts = [carry] + spread(0, carry)[:-1]
        for i in range(rows):
            z = product(tall(work[i] - parts[i]), vcat[i])
            solved[i] = z
            gcat[:, i * width:(i + 1) * width] = tall(z)
        send_end(first_sweep + 1)
        chain(1, solved)
        if first_sweep == 0:
            relay(1)
        carry = incoming(first_sweep + 1)
        parts = spread(1, carry)[1:] + [carry]
        return [work[i] - parts[i] for i in range(rows)]

    def start_halo():
        for direction in range(2):
            @pl.when(sends(direction, 0))
            def _():
                for which in range(2):
                    for t in range(nq):
                        halo_copy(direction, which, t, q, ahead(t)).start()

    lane = lax.broadcasted_iota(jnp.int32, (dirs, width), 1)

    def share(which, adjoint):
        for g in range(groups):
            for dst in range(nq):
                piece = None
                for ii in range(nq):
                    shift = ((ii - dst) * cut) % width
                    x = adjoint[g * nq + ii]
                    x = pltpu.roll(x, shift, 1) if shift else x
                    piece = x if piece is None else jnp.where(lane >= ii * cut, x, piece)
                packed[which, dst, g] = piece
        for t in range(1, nq):
            share_copy(which, t - 1, q, ahead(t)).start()
        copy = pltpu.make_async_copy(
            packed.at[which, q], shares.at[:, which, q], l_sem.at[2 + which])
        copy.start()
        local.append(copy)

    adjoint_two = solve(0, grad_two, start_halo)
    for i in range(rows):
        total = grad_one[i] + adjoint_two[i]
        solved[i] = total
        gcat[:, i * width:(i + 1) * width] = tall(total)
    def pass_on():
        share(1, adjoint_two)
        for which in range(2):
            for t in range(1, pairs):
                state_copy(which, t - 1, behind(2 * t), q).wait_recv()
                state_forward(which, t, behind(2 * t)).start()

    adjoint_one = solve(2, solved, pass_on)
    share(0, adjoint_one)

    for which in range(2):
        for t in range(pairs):
            state_forward(which, t, lax.rem(partner + nq - 2 * t, nq)).wait_recv()
    for direction in range(2):
        @pl.when(gets(direction, 0))
        def _():
            for which in range(2):
                for t in range(nq):
                    halo_copy(direction, which, t, behind(t), q).wait_recv()

        @pl.when(jnp.logical_not(gets(direction, 0)))
        def _():
            slot = 0 if direction == 0 else rows + 1
            states[slot] = jnp.zeros(states.shape[1:], F32)
    for copy in local[:2]:
        copy.wait()

    depth = nq * dirs
    for which in (1, 0):
        for t in range(1, nq):
            share_copy(which, t - 1, behind(t), q).wait_recv()
        local[3 - which].wait()
        part = slice(which * depth, (which + 1) * depth)
        for g in range(groups):
            high, low = halves(jnp.transpose(shares[g, which].reshape(depth, width)))
            lhs[0, g * width:(g + 1) * width, part] = high
            lhs[1, g * width:(g + 1) * width, part] = low
        for j in range(rows + 2):
            low_row, high_row = max(j - 2, 0), min(j, last)
            a, b = low_row * cut, (high_row + 1) * cut
            left = jnp.concatenate([lhs[0, a:b, part], lhs[1, a:b, part]], axis=0)
            r = product(left, wide(states[j, which].reshape(depth, width)))
            for i in range(low_row, high_row + 1):
                piece = {j - 1: 0, j: 1, j - 2: 2}[i]
                place = pl.ds(piece * rows + i, cut, stride=3 * rows)
                term = r[(i - low_row) * cut:(i - low_row + 1) * cut, :]
                out[place, :] = -term if which == 1 else out[place, :] - term

    for which in range(2):
        for t in range(1, pairs):
            state_copy(which, t - 1, q, ahead(2 * t)).wait_send()
        for t in range(pairs):
            state_forward(which, t, behind(2 * t)).wait_send()
        for t in range(1, nq):
            share_copy(which, t - 1, q, ahead(t)).wait_send()
    for direction in range(2):
        @pl.when(sends(direction, 0))
        def _():
            for which in range(2):
                for t in range(nq):
                    halo_copy(direction, which, t, q, ahead(t)).wait_send()

        for k in range(n - 2):
            @pl.when(sends(direction, k))
            def _():
                map_copy(direction, k).wait_send()

            @pl.when(gets(direction, k))
            def _():
                map_forward(direction, k, parity).wait_send()
    for sweep in range(4):
        for k in range(n - 1):
            @pl.when(sends(sweep % 2, k))
            def _():
                end_copy(sweep, k).wait_send()


def body(n, nq, *args):
    rows, dirs, width = args[3].shape
    cut = width // nq
    groups = rows // nq
    depth = 2 * nq * dirs
    dma = pltpu.SemaphoreType.DMA
    vmem = pl.BlockSpec(memory_space=pltpu.VMEM)
    result = pl.pallas_call(
        functools.partial(kernel, n, nq),
        out_shape=jax.ShapeDtypeStruct((cut * 3 * rows, width), F32),
        in_specs=[vmem] * 7,
        out_specs=vmem,
        scratch_shapes=[
            pltpu.VMEM((2, rows, width, 2 * width), BF16),
            pltpu.VMEM((2, rows - 1, width, 2 * width), BF16),
            pltpu.VMEM((2, width, rows * 2 * width), BF16),
            pltpu.VMEM((2, rows * width, 2 * width), BF16),
            pltpu.VMEM((rows, width, 2 * width), BF16),
            pltpu.VMEM((2, (n - 2) * width, 2 * width), BF16),
            pltpu.VMEM((2, width, width), F32),
            pltpu.VMEM((2, n - 2, width, width), F32),
            pltpu.VMEM((4, dirs, width), F32),
            pltpu.VMEM((4, n - 1, dirs, width), F32),
            pltpu.VMEM((2 * dirs, rows * width), BF16),
            pltpu.VMEM((rows, dirs, width), F32),
            pltpu.VMEM((rows, dirs, width), F32),
            pltpu.VMEM((2, nq, groups, dirs, width), F32),
            pltpu.VMEM((groups, 2, nq, dirs, width), F32),
            pltpu.VMEM((rows + 2, 2, nq, dirs, width), F32),
            pltpu.VMEM((2, rows * cut, depth), BF16),
            dma((2, n - 2)), dma((2, n - 2)),
            dma((2, n - 2)), dma((2, n - 2)),
            dma((4, n - 1)), dma((4, n - 1)),
            dma((2, nq - 1)), dma((2, nq - 1)),
            dma((2, max(nq // 2 - 1, 1))), dma((2, max(nq // 2 - 1, 1))),
            dma((2, nq // 2)), dma((2, nq // 2)),
            dma((2, 2, nq)), dma((2, 2, nq)),
            dma((4,)),
        ],
        compiler_params=pltpu.CompilerParams(
            collective_id=0, has_side_effects=True, vmem_limit_bytes=60 * 1024 * 1024),
    )(*args)
    return result.reshape(cut, 3, rows, width)


def solution(mesh):
    factors = P("rows", None, None)
    vectors = P("rows", "rhs", None)
    return jax.shard_map(
        functools.partial(body, mesh.shape["rows"], mesh.shape["rhs"]),
        mesh=mesh,
        in_specs=(factors,) * 3 + (vectors,) * 4,
        out_specs=P("rhs", None, "rows", None),
        check_vma=False,
    )
```
